8 devices in a mesh: data: 1 (over z), stage: 8 (over y, x, core).
Axes of the slice: x: 2, y: 2, z: 1, core: 2. Of those that a mesh axis runs over, the one named last changes fastest.
Arguments:
- x_init: float32 [2, 256, 16], P('data')
- h_warm: bfloat16 [7, 2, 256, 768], P(None, 'data')
- skip_warm: bfloat16 [4, 2, 256, 768], P(None, 'data')
- w_in: bfloat16 [16, 768], replicated
- w_out: bfloat16 [768, 16], replicated
- w_qkv: bfloat16 [8, 768, 2304], P('stage')
- w_o: bfloat16 [8, 12, 64, 768], P('stage')
- w_up: bfloat16 [8, 768, 3072], P('stage')
- w_down: bfloat16 [8, 3072, 768], P('stage')
- w_skip: bfloat16 [4, 1536, 768], replicated
- ada_mods: float32 [32, 8, 6, 768], P(None, 'stage')
- coef_keep: float32 [32], replicated
- coef_noise: float32 [32], replicated
Outputs:
- output: float32 [2, 256, 16], P('data')
All inputs are finite; a program needn't handle non-finite values.
Results may differ from the reference program's by a relative error of at most 0.0137019.
Values are sent between devices in bfloat16 or wider.
A program may use at most 1 GiB of HBM per device.

```python
import jax
import jax.numpy as jnp
from jax import lax
import math

WIDTH = 768
NUM_HEADS = 12
LAYERS = 8
TOKENS = 256
CHANNELS = 16
STAGES = 8
BATCH_PART = 2
NUM_STEPS = 32

HEAD_DIM = WIDTH // NUM_HEADS
PER_STAGE = LAYERS // STAGES
HALF_LAYERS = LAYERS // 2
HALF_STAGES = STAGES // 2
N_ROWS = BATCH_PART * TOKENS
SCORE_SCALE = 1.0 / math.sqrt(HEAD_DIM)
LN_EPS = 1e-6


def setup_inputs(seed: int = 0, part: int = 0) -> dict:
    base_key = jax.random.key(seed)
    weight_keys = jax.random.split(base_key, 10)
    part_keys = jax.random.split(jax.random.fold_in(base_key, part), 3)

    def weight(key_one, array_shape, fan_in):
        return (jax.random.normal(key_one, array_shape, jnp.float32) / math.sqrt(fan_in)).astype(jnp.bfloat16)

    x_init = jax.random.normal(part_keys[0], (BATCH_PART, TOKENS, CHANNELS), jnp.float32)
    h_warm = jax.random.normal(part_keys[1], (STAGES - 1, BATCH_PART, TOKENS, WIDTH), jnp.float32).astype(jnp.bfloat16)
    skip_warm = jax.random.normal(part_keys[2], (HALF_LAYERS, BATCH_PART, TOKENS, WIDTH), jnp.float32).astype(jnp.bfloat16)
    gate_mean = jnp.array([0.0, 0.0, 0.6, 0.0, 0.0, 0.6], dtype=jnp.float32).reshape(1, 1, 6, 1)
    ada_mods = gate_mean + 0.2 * jax.random.normal(weight_keys[7], (NUM_STEPS, LAYERS, 6, WIDTH), jnp.float32)
    return dict(
        x_init=x_init,
        h_warm=h_warm,
        skip_warm=skip_warm,
        w_in=weight(weight_keys[0], (CHANNELS, WIDTH), CHANNELS),
        w_out=weight(weight_keys[1], (WIDTH, CHANNELS), WIDTH),
        w_qkv=weight(weight_keys[2], (LAYERS, WIDTH, 3 * WIDTH), WIDTH),
        w_o=weight(weight_keys[3], (LAYERS, NUM_HEADS, HEAD_DIM, WIDTH), WIDTH),
        w_up=weight(weight_keys[4], (LAYERS, WIDTH, 4 * WIDTH), WIDTH),
        w_down=weight(weight_keys[5], (LAYERS, 4 * WIDTH, WIDTH), 4 * WIDTH),
        w_skip=weight(weight_keys[6], (HALF_LAYERS, 2 * WIDTH, WIDTH), 2 * WIDTH),
        ada_mods=ada_mods,
        coef_keep=jax.random.uniform(weight_keys[8], (NUM_STEPS,), jnp.float32, 0.7, 0.95),
        coef_noise=-jax.random.uniform(weight_keys[9], (NUM_STEPS,), jnp.float32, 0.2, 0.5),
    )


def layer_norm(hidden):
    centered = hidden - jnp.mean(hidden, axis=-1, keepdims=True)
    variance = jnp.mean(centered * centered, axis=-1, keepdims=True)
    return centered * lax.rsqrt(variance + LN_EPS)


def attention_one(qkv_one):
    queries = qkv_one[:, 0].astype(jnp.float32)
    key_rows = qkv_one[:, 1].astype(jnp.float32)
    value_rows = qkv_one[:, 2].astype(jnp.float32)
    scores = jnp.einsum('qhd,khd->hqk', queries, key_rows) * SCORE_SCALE
    attn_probs = jax.nn.softmax(scores, axis=-1).astype(jnp.bfloat16).astype(jnp.float32)
    return jnp.einsum('hqk,khd->qhd', attn_probs, value_rows).astype(jnp.bfloat16)


def dit_block(hidden, block_mod, wqkv_one, wo_one, wup_one, wdown_one):
    normed = layer_norm(hidden) * (1.0 + block_mod[1]) + block_mod[0]
    qkv_all = jnp.dot(normed.astype(jnp.bfloat16).reshape(N_ROWS, WIDTH), wqkv_one, preferred_element_type=jnp.float32).astype(jnp.bfloat16)
    attended = lax.map(attention_one, qkv_all.reshape(BATCH_PART, TOKENS, 3, NUM_HEADS, HEAD_DIM))
    attn_out = jnp.dot(attended.reshape(N_ROWS, WIDTH), wo_one.reshape(WIDTH, WIDTH), preferred_element_type=jnp.float32)
    hidden = hidden + block_mod[2] * attn_out.reshape(BATCH_PART, TOKENS, WIDTH)
    normed = layer_norm(hidden) * (1.0 + block_mod[4]) + block_mod[3]
    mlp_hidden = jnp.dot(normed.astype(jnp.bfloat16).reshape(N_ROWS, WIDTH), wup_one, preferred_element_type=jnp.float32)
    gelu_act = jax.nn.gelu(mlp_hidden, approximate=True).astype(jnp.bfloat16)
    mlp_out = jnp.dot(gelu_act, wdown_one, preferred_element_type=jnp.float32)
    return hidden + block_mod[5] * mlp_out.reshape(BATCH_PART, TOKENS, WIDTH)


def skip_project(hidden, skip_one, wskip_one):
    main_part = jnp.dot(hidden.astype(jnp.bfloat16).reshape(N_ROWS, WIDTH), wskip_one[:WIDTH], preferred_element_type=jnp.float32)
    skip_part = jnp.dot(skip_one.reshape(N_ROWS, WIDTH), wskip_one[WIDTH:], preferred_element_type=jnp.float32)
    return (main_part + skip_part).reshape(BATCH_PART, TOKENS, WIDTH)


def reference(x_init, h_warm, skip_warm, w_in, w_out, w_qkv, w_o, w_up, w_down, w_skip, ada_mods, coef_keep, coef_noise):
    def run_stage(stage_in, stage_id, step_mods, skip_in):
        skip_for = jnp.flip(skip_in, 0)

        def layer_body(hidden, offset):
            block_id = stage_id * PER_STAGE + offset
            skip_id = jnp.maximum(block_id - HALF_LAYERS, 0)
            projected = skip_project(hidden, skip_for[skip_id], w_skip[skip_id])
            hidden = jnp.where(block_id >= HALF_LAYERS, projected, hidden)
            hidden = dit_block(hidden, step_mods[block_id], w_qkv[block_id], w_o[block_id], w_up[block_id], w_down[block_id])
            return hidden, hidden.astype(jnp.bfloat16)

        return lax.scan(layer_body, stage_in, jnp.arange(PER_STAGE))[1]

    def step_body(state_in, step_in):
        latent, bound_in, skip_in = state_in
        step_mods, keep_one, noise_one = step_in
        from_latent = jnp.dot(latent.astype(jnp.bfloat16).reshape(N_ROWS, CHANNELS), w_in, preferred_element_type=jnp.float32).reshape(BATCH_PART, TOKENS, WIDTH)
        stage_ins = jnp.concatenate([from_latent[None], bound_in.astype(jnp.float32)], axis=0)

        def stage_fn(stage_pair):
            return run_stage(stage_pair[0], stage_pair[1], step_mods, skip_in)

        block_outs = lax.map(stage_fn, (stage_ins, jnp.arange(STAGES)))
        last_out = block_outs[STAGES - 1, PER_STAGE - 1]
        noise_pred = jnp.dot(last_out.reshape(N_ROWS, WIDTH), w_out, preferred_element_type=jnp.float32).reshape(BATCH_PART, TOKENS, CHANNELS)
        new_latent = keep_one * latent + noise_one * noise_pred
        new_bound = block_outs[:STAGES - 1, PER_STAGE - 1]
        new_skips = block_outs[:HALF_STAGES].reshape(HALF_LAYERS, BATCH_PART, TOKENS, WIDTH)
        return (new_latent, new_bound, new_skips), None

    final_state = lax.scan(step_body, (x_init, h_warm, skip_warm), (ada_mods, coef_keep, coef_noise))[0]
    return final_state[0]
```

```python
import math

import jax
import jax.numpy as jnp
from jax import lax
from jax.experimental import pallas as pl
from jax.experimental.pallas import tpu as pltpu
from jax.sharding import PartitionSpec as P

MESH = pl.DeviceIdType.MESH
F32, BF16 = jnp.float32, jnp.bfloat16
STEPS, ROWS, WIDTH, HEADS, CHANNELS = 32, 256, 768, 12, 16
QKV, HIDDEN = 3 * WIDTH, 4 * WIDTH
SLOTS = 4
NCH = 256
EXP_SCALE = (1.0 / math.sqrt(WIDTH // HEADS)) * math.log2(math.e)
GELU_A = math.sqrt(2.0 / math.pi)
GELU_B = 0.044715 * math.sqrt(2.0 / math.pi)
MOVES = ((0, 2, 0), (2, 4, 0), (3, 6, 0), (4, 7, 1), (6, 0, 1), (7, 3, 1))
STAYS = ((1, 0), (5, 1))
PIECES = ((4, 0, STEPS), (0, 0, WIDTH), (1, 0, WIDTH), (2, 0, WIDTH),
          (3, 0, WIDTH), (3, WIDTH, WIDTH), (3, 2 * WIDTH, WIDTH), (3, 3 * WIDTH, WIDTH))


def pick(index, values):
    out = jnp.int32(values[0])
    for n, value in enumerate(values[1:], 1):
        out = jnp.where(index == n, jnp.int32(value), out)
    return out


def dot(a, b):
    return jnp.dot(a, b, preferred_element_type=F32)


def layer_norm(h, scale, shift):
    mean = jnp.mean(h, axis=-1, keepdims=True)
    cen = h - mean
    var = jnp.mean(cen * cen, axis=-1, keepdims=True)
    return (cen * lax.rsqrt(var + 1e-6) * scale + shift).astype(BF16)


def gelu(x):
    return (0.5 * x) * (1.0 + jnp.tanh(x * (GELU_A + GELU_B * (x * x))))


def kernel(x_ref, hw_ref, sw_ref, win_ref, wout_ref, wqkv_ref, wo_ref, wup_ref, wdown_ref, wskip_ref, mods_ref,
           keep_ref, noise_ref, out_ref, wq, wo, wu, wd, ws, md, chain, outb, h_ref, u_ref, qkv_ref, att_ref,
           act_ref, lat_ref, latt_ref, fin_ref, wsend, wfwd, wrecv, csend, crecv, lsem, fsend, frecv):
    me = lax.axis_index('stage')
    core = lax.rem(me, 2)
    chip = lax.div(me, 2)
    pos = pick(chip, (1, 0, 2, 3))
    next_dev = pick(chip, (2, 0, 3, 3)) * 2 + core
    prev_dev = pick(chip, (1, 1, 0, 2)) * 2 + core
    partner = me + 1 - 2 * core
    first_kind = pick(me, (1, 0, 0, 1, 0, 1, 0, 1))

    held = (wq, wo, wu, wd, md)
    given = (wqkv_ref, wo_ref, wup_ref, wdown_ref, mods_ref)

    def remote(src, dst, send, recv, dev):
        return pltpu.make_async_remote_copy(src_ref=src, dst_ref=dst, send_sem=send, recv_sem=recv,
                                            device_id={'stage': dev}, device_id_type=MESH)

    def source(n):
        arr, row, size = PIECES[n]
        return given[arr].at[pl.ds(row, size)]

    def target(n, kind):
        arr, row, size = PIECES[n]
        return held[arr].at[kind, pl.ds(row, size)]

    for src, dst, kind in MOVES:
        @pl.when(me == src)
        def _():
            for n in range(len(PIECES)):
                remote(source(n), target(n, kind), wsend.at[n], wrecv.at[kind, n], jnp.int32(dst)).start()
    for src, kind in STAYS:
        @pl.when(me == src)
        def _():
            for n in range(len(PIECES)):
                pltpu.make_async_copy(source(n), target(n, kind), wrecv.at[kind, n]).start()

    locals_ = [
        pltpu.make_async_copy(wskip_ref.at[3 - pos], ws, lsem.at[0]),
        pltpu.make_async_copy(hw_ref.at[jnp.maximum(pos - 1, 0), core], chain.at[0, 0], lsem.at[1]),
        pltpu.make_async_copy(hw_ref.at[6 - pos, core], chain.at[1, 0], lsem.at[2]),
        pltpu.make_async_copy(sw_ref.at[pos, core], outb.at[0, SLOTS - 1], lsem.at[3]),
    ]
    for copy in locals_:
        copy.start()
    lat_ref[0] = x_ref[core]
    for copy in locals_:
        copy.wait()

    def piece_copy(n, kind):
        return remote(target(n, kind), target(n, kind), wfwd.at[n], wrecv.at[kind, n], partner)

    for n in range(len(PIECES)):
        for kind in range(2):
            @pl.when(first_kind == kind)
            def _():
                piece_copy(n, kind).wait_recv()
                piece_copy(n, kind).start()
    for n in range(len(PIECES)):
        for kind in range(2):
            @pl.when(first_kind != kind)
            def _():
                piece_copy(n, kind).wait_recv()

    def chain_copy(kind, k, lo, size, dev):
        s, r = lax.rem(k, SLOTS), lax.rem(k + 1, SLOTS)
        return remote(outb.at[kind, s, :, pl.ds(lo, size)], chain.at[kind, r, :, pl.ds(lo, size)],
                      csend.at[kind, s], crecv.at[kind, r], dev)

    low = lax.broadcasted_iota(jnp.int32, (ROWS, 128), 1) < 64

    def split(pair):
        zero = jnp.zeros_like(pair)
        return jnp.where(low, pair, zero), jnp.where(low, zero, pair)

    def item(j, _):
        k = lax.div(j, 2)
        kind = lax.rem(j + core, 2)
        slot = lax.rem(k, SLOTS)
        dest = jnp.where(kind == 0, next_dev, prev_dev)
        has_dest = jnp.where(kind == 0, pos < 3, pos > 0)
        has_src = jnp.where(kind == 0, pos > 0, pos < 3)
        sends = jnp.logical_and(has_dest, k < STEPS - 2 + kind)

        @pl.when(jnp.logical_and(has_dest, k >= SLOTS))
        def _():
            chain_copy(kind, k, 0, WIDTH, dest).wait_send()

        @pl.when(jnp.logical_and(has_src, k > 0))
        def _():
            chain_copy(kind, k + SLOTS - 1, 0, WIDTH, dest).wait_recv()

        @pl.when(jnp.logical_and(kind == 0, pos == 0))
        def _():
            x = lat_ref[lax.rem(k, 2)].astype(BF16)
            h_ref[...] = dot(x, win_ref[...])

        @pl.when(jnp.logical_and(kind == 0, pos > 0))
        def _():
            h_ref[...] = chain[0, slot].astype(F32)

        @pl.when(kind == 1)
        def _():
            zslot = lax.rem(k + SLOTS - 1, SLOTS)
            for n in range(0, WIDTH, NCH):
                h_ref[:, n:n + NCH] = (dot(chain[1, slot], ws[:WIDTH, n:n + NCH])
                                       + dot(outb[0, zslot], ws[WIDTH:, n:n + NCH]))

        def mod(index):
            return md[kind, k, index:index + 1, :]

        for r in range(0, ROWS, 64):
            u_ref[r:r + 64] = layer_norm(h_ref[r:r + 64], 1.0 + mod(1), mod(0))
        for n in range(0, QKV, NCH):
            qkv_ref[:, n:n + NCH] = dot(u_ref[...], wq[kind, :, n:n + NCH]).astype(BF16)
        for pair in range(HEADS // 2):
            c = pair * 128
            qa, qb = split(qkv_ref[:, c:c + 128])
            keys = qkv_ref[:, WIDTH + c:WIDTH + c + 128]
            va, vb = split(qkv_ref[:, 2 * WIDTH + c:2 * WIDTH + c + 128])
            total = None
            for q, v in ((qa, va), (qb, vb)):
                s = lax.dot_general(q, keys, (((1,), (1,)), ((), ())), preferred_element_type=F32)
                e = jnp.exp2((s - jnp.max(s, axis=-1, keepdims=True)) * EXP_SCALE)
                a = (e * (1.0 / jnp.sum(e, axis=-1, keepdims=True))).astype(BF16)
                o = dot(a, v)
                total = o if total is None else total + o
            att_ref[:, c:c + 128] = total.astype(BF16)
        for n in range(0, WIDTH, NCH):
            h_ref[:, n:n + NCH] += mod(2)[:, n:n + NCH] * dot(att_ref[...], wo[kind, :, n:n + NCH])
        for r in range(0, ROWS, 64):
            u_ref[r:r + 64] = layer_norm(h_ref[r:r + 64], 1.0 + mod(4), mod(3))
        for n in range(0, HIDDEN, NCH):
            act_ref[:, n:n + NCH] = gelu(dot(u_ref[...], wu[kind, :, n:n + NCH])).astype(BF16)
        for n in range(0, WIDTH, NCH):
            new = h_ref[:, n:n + NCH] + mod(5)[:, n:n + NCH] * dot(act_ref[...], wd[kind, :, n:n + NCH])
            outb[kind, slot, :, n:n + NCH] = new.astype(BF16)

            @pl.when(sends)
            def _():
                chain_copy(kind, k, n, NCH, dest).start()

        @pl.when(jnp.logical_and(kind == 0, pos == 3))
        def _():
            chain[1, lax.rem(k + 1, SLOTS)] = outb[0, slot]

        @pl.when(jnp.logical_and(kind == 1, pos == 0))
        def _():
            eps = dot(outb[1, slot], wout_ref[...])
            lat_ref[lax.rem(k + 1, 2)] = keep_ref[k] * lat_ref[lax.rem(k, 2)] + noise_ref[k] * eps
        return 0

    def guarded(j, carry):
        skipped = jnp.logical_and(lax.div(j, 2) == STEPS - 1, lax.rem(j + core, 2) == 0)

        @pl.when(jnp.logical_not(skipped))
        def _():
            item(j, 0)
        return carry

    lax.fori_loop(0, 2 * STEPS, guarded, 0)

    for kind, first, last in ((0, STEPS - 5, STEPS - 3), (1, STEPS - 4, STEPS - 2)):
        for k in range(first, last + 1):
            @pl.when(pos < 3 if kind == 0 else pos > 0)
            def _():
                chain_copy(kind, jnp.int32(k), 0, WIDTH, me).wait_send()

    for src, dst, kind in MOVES:
        @pl.when(me == src)
        def _():
            for n in range(len(PIECES)):
                remote(source(n), target(n, kind), wsend.at[n], wrecv.at[kind, n], jnp.int32(dst)).wait_send()
    for n in range(len(PIECES)):
        piece_copy(n, first_kind).wait_send()

    def final_copy(sample, dev):
        return remote(latt_ref, fin_ref.at[sample], fsend.at[dev], frecv.at[sample], jnp.int32(dev))

    for sample in range(2):
        @pl.when(me == 2 + sample)
        def _():
            latt_ref[...] = lat_ref[STEPS % 2].T
            for dev in range(8):
                if dev != 2 + sample:
                    final_copy(sample, dev).start()
            for dev in range(8):
                if dev != 2 + sample:
                    final_copy(sample, dev).wait_send()
            out_ref[sample] = lat_ref[STEPS % 2]

        @pl.when(me != 2 + sample)
        def _():
            final_copy(sample, 0).wait_recv()
            out_ref[sample] = fin_ref[sample].T


def solution(mesh):
    assert mesh.shape['stage'] == 8

    def local_run(x_init, h_warm, skip_warm, w_in, w_out, w_qkv, w_o, w_up, w_down, w_skip, ada_mods, keep, noise):
        vmem, hbm, smem = (pl.BlockSpec(memory_space=s) for s in (pltpu.VMEM, pl.ANY, pltpu.SMEM))
        npieces = len(PIECES)
        dma = pltpu.SemaphoreType.DMA
        return pl.pallas_call(
            kernel,
            out_shape=jax.ShapeDtypeStruct(x_init.shape, F32),
            in_specs=[vmem, hbm, hbm, vmem, vmem, hbm, hbm, hbm, hbm, hbm, hbm, smem, smem],
            out_specs=vmem,
            scratch_shapes=[
                pltpu.VMEM((2, WIDTH, QKV), BF16), pltpu.VMEM((2, WIDTH, WIDTH), BF16),
                pltpu.VMEM((2, WIDTH, HIDDEN), BF16), pltpu.VMEM((2, HIDDEN, WIDTH), BF16),
                pltpu.VMEM((2 * WIDTH, WIDTH), BF16), pltpu.VMEM((2, STEPS, 6, WIDTH), F32),
                pltpu.VMEM((2, SLOTS, ROWS, WIDTH), BF16), pltpu.VMEM((2, SLOTS, ROWS, WIDTH), BF16),
                pltpu.VMEM((ROWS, WIDTH), F32), pltpu.VMEM((ROWS, WIDTH), BF16), pltpu.VMEM((ROWS, QKV), BF16),
                pltpu.VMEM((ROWS, WIDTH), BF16), pltpu.VMEM((ROWS, HIDDEN), BF16),
                pltpu.VMEM((2, ROWS, CHANNELS), F32), pltpu.VMEM((CHANNELS, ROWS), F32),
                pltpu.VMEM((2, CHANNELS, ROWS), F32),
                dma((npieces,)), dma((npieces,)), dma((2, npieces)), dma((2, SLOTS)), dma((2, SLOTS)),
                dma((4,)), dma((8,)), dma((2,)),
            ],
            compiler_params=pltpu.CompilerParams(has_side_effects=True, vmem_limit_bytes=63 * 1024 * 1024),
        )(x_init, h_warm, skip_warm, w_in, w_out, w_qkv[0], w_o[0].reshape(WIDTH, WIDTH), w_up[0], w_down[0], w_skip,
          ada_mods[:, 0], keep, noise)

    in_specs = (P('data'), P(None, 'data'), P(None, 'data'), P(), P(), P('stage'), P('stage'), P('stage'), P('stage'),
                P(), P(None, 'stage'), P(), P())
    return jax.shard_map(local_run, mesh=mesh, in_specs=in_specs, out_specs=P('data'), check_vma=False)
```

```python
import math

import jax
import jax.numpy as jnp
from jax import lax
from jax.experimental import pallas as pl
from jax.experimental.pallas import tpu as pltpu
from jax.sharding import PartitionSpec as P

MESH = pl.DeviceIdType.MESH
F32, BF16 = jnp.float32, jnp.bfloat16
STEPS, ROWS, WIDTH, HEADS, CHANNELS = 32, 256, 768, 12, 16
QKV, HIDDEN = 3 * WIDTH, 4 * WIDTH
SLOTS = 4
NCH = 256
LN_ROWS = 32
EXP_SCALE = (1.0 / math.sqrt(WIDTH // HEADS)) * math.log2(math.e)
GELU_A = math.sqrt(2.0 / math.pi)
GELU_B = 0.044715 * math.sqrt(2.0 / math.pi)
MOVES = ((0, 2, 0), (2, 4, 0), (3, 6, 0), (4, 7, 1), (6, 0, 1), (7, 3, 1))
STAYS = ((1, 0), (5, 1))
PIECES = ((4, 0, STEPS), (0, 0, WIDTH), (1, 0, WIDTH), (2, 0, WIDTH),
          (3, 0, WIDTH), (3, WIDTH, WIDTH), (3, 2 * WIDTH, WIDTH), (3, 3 * WIDTH, WIDTH))


def pick(index, values):
    out = jnp.int32(values[0])
    for n, value in enumerate(values[1:], 1):
        out = jnp.where(index == n, jnp.int32(value), out)
    return out


def dot(a, b):
    return jnp.dot(a, b, preferred_element_type=F32)


def dot_t(a, b):
    return lax.dot_general(a, b, (((1,), (1,)), ((), ())), preferred_element_type=F32)


def fold(op, x):
    while x.shape[0] > 8:
        half = x.shape[0] // 2
        x = op(x[:half], x[half:])
    reduce = jnp.max if op is jnp.maximum else jnp.sum
    return reduce(x, axis=0, keepdims=True)


def layer_norm(h, scale, shift):
    mean = jnp.mean(h, axis=-1, keepdims=True)
    cen = h - mean
    var = jnp.mean(cen * cen, axis=-1, keepdims=True)
    return (cen * lax.rsqrt(var + 1e-6) * scale + shift).astype(BF16)


def gelu(x):
    return (0.5 * x) * (1.0 + jnp.tanh(x * (GELU_A + GELU_B * (x * x))))


def kernel(x_ref, hw_ref, sw_ref, win_ref, wout_ref, wqkv_ref, wo_ref, wup_ref, wdown_ref, wskip_ref, mods_ref,
           keep_ref, noise_ref, out_ref, wq, wo, wu, wd, ws, md, chain, outb, wv, h_ref, u_ref, qk_ref, vt_ref, st_ref, att_ref,
           act_ref, lat_ref, latt_ref, fin_ref, wsend, wfwd, wrecv, csend, crecv, lsem, fsend, frecv):
    me = lax.axis_index('stage')
    core = lax.rem(me, 2)
    chip = lax.div(me, 2)
    pos = pick(chip, (1, 0, 2, 3))
    next_dev = pick(chip, (2, 0, 3, 3)) * 2 + core
    prev_dev = pick(chip, (1, 1, 0, 2)) * 2 + core
    partner = me + 1 - 2 * core
    first_kind = pick(me, (1, 0, 0, 1, 0, 1, 0, 1))

    held = (wq, wo, wu, wd, md)
    given = (wqkv_ref, wo_ref, wup_ref, wdown_ref, mods_ref)

    def remote(src, dst, send, recv, dev):
        return pltpu.make_async_remote_copy(src_ref=src, dst_ref=dst, send_sem=send, recv_sem=recv,
                                            device_id={'stage': dev}, device_id_type=MESH)

    def source(n):
        arr, row, size = PIECES[n]
        return given[arr].at[pl.ds(row, size)]

    def target(n, kind):
        arr, row, size = PIECES[n]
        return held[arr].at[kind, pl.ds(row, size)]

    for src, dst, kind in MOVES:
        @pl.when(me == src)
        def _():
            for n in range(len(PIECES)):
                remote(source(n), target(n, kind), wsend.at[n], wrecv.at[kind, n], jnp.int32(dst)).start()
    for src, kind in STAYS:
        @pl.when(me == src)
        def _():
            for n in range(len(PIECES)):
                pltpu.make_async_copy(source(n), target(n, kind), wrecv.at[kind, n]).start()

    locals_ = [
        pltpu.make_async_copy(wskip_ref.at[3 - pos], ws, lsem.at[0]),
        pltpu.make_async_copy(hw_ref.at[jnp.maximum(pos - 1, 0), core], chain.at[0, 0], lsem.at[1]),
        pltpu.make_async_copy(hw_ref.at[6 - pos, core], chain.at[1, 0], lsem.at[2]),
        pltpu.make_async_copy(sw_ref.at[pos, core], outb.at[0, SLOTS - 1], lsem.at[3]),
    ]
    for copy in locals_:
        copy.start()
    lat_ref[0] = x_ref[core]
    for copy in locals_:
        copy.wait()

    def piece_copy(n, kind):
        return remote(target(n, kind), target(n, kind), wfwd.at[n], wrecv.at[kind, n], partner)

    for n in range(len(PIECES)):
        for kind in range(2):
            @pl.when(first_kind == kind)
            def _():
                piece_copy(n, kind).wait_recv()
                piece_copy(n, kind).start()
    for n in range(len(PIECES)):
        for kind in range(2):
            @pl.when(first_kind != kind)
            def _():
                piece_copy(n, kind).wait_recv()

    for kind in range(2):
        for n in range(0, WIDTH, NCH):
            wv[kind, n:n + NCH] = wq[kind, :, 2 * WIDTH + n:2 * WIDTH + n + NCH].T

    def chain_copy(kind, k, lo, size, dev):
        s, r = lax.rem(k, SLOTS), lax.rem(k + 1, SLOTS)
        return remote(outb.at[kind, s, :, pl.ds(lo, size)], chain.at[kind, r, :, pl.ds(lo, size)],
                      csend.at[kind, s], crecv.at[kind, r], dev)

    low = lax.broadcasted_iota(jnp.int32, (ROWS, 128), 1) < 64

    def split(pair):
        zero = jnp.zeros_like(pair)
        return jnp.where(low, pair, zero), jnp.where(low, zero, pair)

    def item(j, _):
        k = lax.div(j, 2)
        kind = lax.rem(j + core, 2)
        slot = lax.rem(k, SLOTS)
        dest = jnp.where(kind == 0, next_dev, prev_dev)
        has_dest = jnp.where(kind == 0, pos < 3, pos > 0)
        has_src = jnp.where(kind == 0, pos > 0, pos < 3)
        sends = jnp.logical_and(has_dest, k < STEPS - 2 + kind)

        @pl.when(jnp.logical_and(has_dest, k >= SLOTS))
        def _():
            chain_copy(kind, k, 0, WIDTH, dest).wait_send()

        @pl.when(jnp.logical_and(has_src, k > 0))
        def _():
            chain_copy(kind, k + SLOTS - 1, 0, WIDTH, dest).wait_recv()

        @pl.when(jnp.logical_and(kind == 0, pos == 0))
        def _():
            x = lat_ref[lax.rem(k, 2)].astype(BF16)
            h_ref[...] = dot(x, win_ref[...])

        @pl.when(jnp.logical_and(kind == 0, pos > 0))
        def _():
            h_ref[...] = chain[0, slot].astype(F32)

        @pl.when(kind == 1)
        def _():
            zslot = lax.rem(k + SLOTS - 1, SLOTS)
            for n in range(0, WIDTH, NCH):
                h_ref[:, n:n + NCH] = (dot(chain[1, slot], ws[:WIDTH, n:n + NCH])
                                       + dot(outb[0, zslot], ws[WIDTH:, n:n + NCH]))

        def mod(index):
            return md[kind, k, index:index + 1, :]

        for r in range(0, ROWS, LN_ROWS):
            u_ref[r:r + LN_ROWS] = layer_norm(h_ref[r:r + LN_ROWS], 1.0 + mod(1), mod(0))
        def weights(part):
            e = jnp.exp2((part - fold(jnp.maximum, part)) * EXP_SCALE)
            return e.astype(BF16), 1.0 / fold(jnp.add, e)

        for n in range(0, 2 * WIDTH, NCH):
            qk_ref[:, n:n + NCH] = dot(u_ref[...], wq[kind, :, n:n + NCH]).astype(BF16)
        for n in range(0, WIDTH, NCH):
            vt_ref[n:n + NCH] = dot_t(wv[kind, n:n + NCH], u_ref[...]).astype(BF16)
        for pair in range(HEADS // 2):
            c = pair * 128
            for half, keys in enumerate(split(qk_ref[:, WIDTH + c:WIDTH + c + 128])):
                st_ref[2 * pair + half] = dot_t(keys, qk_ref[:, c:c + 128])

        @pl.when(j >= 0)
        def _():
            for pair in range(HEADS // 2):
                outs = []
                for head in (2 * pair, 2 * pair + 1):
                    parts = [weights(st_ref[head, :, q:q + 128]) for q in (0, 128)]
                    probs = jnp.concatenate([part[0] for part in parts], axis=1)
                    outs.append(dot(vt_ref[head * 64:head * 64 + 64], probs)
                                * jnp.concatenate([part[1] for part in parts], axis=1))
                att_ref[pair] = jnp.concatenate(outs, axis=0).T.astype(BF16)
            att = jnp.concatenate([att_ref[pair] for pair in range(HEADS // 2)], axis=1)
            for n in range(0, WIDTH, NCH):
                h_ref[:, n:n + NCH] += mod(2)[:, n:n + NCH] * dot(att, wo[kind, :, n:n + NCH])
            for r in range(0, ROWS, LN_ROWS):
                u_ref[r:r + LN_ROWS] = layer_norm(h_ref[r:r + LN_ROWS], 1.0 + mod(4), mod(3))
            for n in range(0, HIDDEN, NCH):
                act_ref[:, n:n + NCH] = gelu(dot(u_ref[...], wu[kind, :, n:n + NCH])).astype(BF16)
            for n in range(0, WIDTH, NCH):
                gate = mod(5)[:, n:n + NCH]
                new = h_ref[:, n:n + NCH] + gate * dot(act_ref[:, :HIDDEN // 2], wd[kind, :HIDDEN // 2, n:n + NCH])
                new += gate * dot(act_ref[:, HIDDEN // 2:], wd[kind, HIDDEN // 2:, n:n + NCH])
                outb[kind, slot, :, n:n + NCH] = new.astype(BF16)

        @pl.when(sends)
        def _():
            for n in range(0, WIDTH, NCH):
                chain_copy(kind, k, n, NCH, dest).start()

        @pl.when(jnp.logical_and(kind == 0, pos == 3))
        def _():
            chain[1, lax.rem(k + 1, SLOTS)] = outb[0, slot]

        @pl.when(jnp.logical_and(kind == 1, pos == 0))
        def _():
            eps = dot(outb[1, slot], wout_ref[...])
            lat_ref[lax.rem(k + 1, 2)] = keep_ref[k] * lat_ref[lax.rem(k, 2)] + noise_ref[k] * eps
        return 0

    def guarded(j, carry):
        skipped = jnp.logical_and(lax.div(j, 2) == STEPS - 1, lax.rem(j + core, 2) == 0)

        @pl.when(jnp.logical_not(skipped))
        def _():
            item(j, 0)
        return carry

    lax.fori_loop(0, 2 * STEPS, guarded, 0)

    for kind, first, last in ((0, STEPS - 5, STEPS - 3), (1, STEPS - 4, STEPS - 2)):
        for k in range(first, last + 1):
            @pl.when(pos < 3 if kind == 0 else pos > 0)
            def _():
                chain_copy(kind, jnp.int32(k), 0, WIDTH, me).wait_send()

    for src, dst, kind in MOVES:
        @pl.when(me == src)
        def _():
            for n in range(len(PIECES)):
                remote(source(n), target(n, kind), wsend.at[n], wrecv.at[kind, n], jnp.int32(dst)).wait_send()
    for n in range(len(PIECES)):
        piece_copy(n, first_kind).wait_send()

    def final_copy(sample, dev):
        return remote(latt_ref, fin_ref.at[sample], fsend.at[dev], frecv.at[sample], jnp.int32(dev))

    for sample in range(2):
        @pl.when(me == 2 + sample)
        def _():
            latt_ref[...] = lat_ref[STEPS % 2].T
            for dev in range(8):
                if dev != 2 + sample:
                    final_copy(sample, dev).start()
            for dev in range(8):
                if dev != 2 + sample:
                    final_copy(sample, dev).wait_send()
            out_ref[sample] = lat_ref[STEPS % 2]

        @pl.when(me != 2 + sample)
        def _():
            final_copy(sample, 0).wait_recv()
            out_ref[sample] = fin_ref[sample].T


def solution(mesh):
    assert mesh.shape['stage'] == 8

    def local_run(x_init, h_warm, skip_warm, w_in, w_out, w_qkv, w_o, w_up, w_down, w_skip, ada_mods, keep, noise):
        vmem, hbm, smem = (pl.BlockSpec(memory_space=s) for s in (pltpu.VMEM, pl.ANY, pltpu.SMEM))
        npieces = len(PIECES)
        dma = pltpu.SemaphoreType.DMA
        return pl.pallas_call(
            kernel,
            out_shape=jax.ShapeDtypeStruct(x_init.shape, F32),
            in_specs=[vmem, hbm, hbm, vmem, vmem, hbm, hbm, hbm, hbm, hbm, hbm, smem, smem],
            out_specs=vmem,
            scratch_shapes=[
                pltpu.VMEM((2, WIDTH, QKV), BF16), pltpu.VMEM((2, WIDTH, WIDTH), BF16),
                pltpu.VMEM((2, WIDTH, HIDDEN), BF16), pltpu.VMEM((2, HIDDEN, WIDTH), BF16),
                pltpu.VMEM((2 * WIDTH, WIDTH), BF16), pltpu.VMEM((2, STEPS, 6, WIDTH), F32),
                pltpu.VMEM((2, SLOTS, ROWS, WIDTH), BF16), pltpu.VMEM((2, SLOTS, ROWS, WIDTH), BF16),
                pltpu.VMEM((2, WIDTH, WIDTH), BF16),
                pltpu.VMEM((ROWS, WIDTH), F32), pltpu.VMEM((ROWS, WIDTH), BF16), pltpu.VMEM((ROWS, 2 * WIDTH), BF16),
                pltpu.VMEM((WIDTH, ROWS), BF16), pltpu.VMEM((HEADS, ROWS, ROWS), F32),
                pltpu.VMEM((HEADS // 2, ROWS, 128), BF16), pltpu.VMEM((ROWS, HIDDEN), BF16),
                pltpu.VMEM((2, ROWS, CHANNELS), F32), pltpu.VMEM((CHANNELS, ROWS), F32),
                pltpu.VMEM((2, CHANNELS, ROWS), F32),
                dma((npieces,)), dma((npieces,)), dma((2, npieces)), dma((2, SLOTS)), dma((2, SLOTS)),
                dma((4,)), dma((8,)), dma((2,)),
            ],
            compiler_params=pltpu.CompilerParams(has_side_effects=True, vmem_limit_bytes=63 * 1024 * 1024),
        )(x_init, h_warm, skip_warm, w_in, w_out, w_qkv[0], w_o[0].reshape(WIDTH, WIDTH), w_up[0], w_down[0], w_skip,
          ada_mods[:, 0], keep, noise)

    in_specs = (P('data'), P(None, 'data'), P(None, 'data'), P(), P(), P('stage'), P('stage'), P('stage'), P('stage'),
                P(), P(None, 'stage'), P(), P())
    return jax.shard_map(local_run, mesh=mesh, in_specs=in_specs, out_specs=P('data'), check_vma=False)
```

```python
import math

import jax
import jax.numpy as jnp
from jax import lax
from jax.experimental import pallas as pl
from jax.experimental.pallas import tpu as pltpu
from jax.sharding import PartitionSpec as P

MESH = pl.DeviceIdType.MESH
F32, BF16 = jnp.float32, jnp.bfloat16
STEPS, ROWS, WIDTH, HEADS, CHANNELS = 32, 256, 768, 12, 16
QKV, HIDDEN = 3 * WIDTH, 4 * WIDTH
SLOTS = 4
NCH = 256
LN_ROWS = 32
EXP_SCALE = (1.0 / math.sqrt(WIDTH // HEADS)) * math.log2(math.e)
GELU_A = math.sqrt(2.0 / math.pi)
GELU_B = 0.044715 * math.sqrt(2.0 / math.pi)
MOVES = ((0, 2, 0), (2, 4, 0), (3, 6, 0), (4, 7, 1), (6, 0, 1), (7, 3, 1))
STAYS = ((1, 0), (5, 1))
EARLY = 2 * 6
PIECES = ((4, 0, EARLY), (0, 0, WIDTH), (1, 0, WIDTH), (2, 0, WIDTH), (3, 0, WIDTH), (3, WIDTH, WIDTH),
          (3, 2 * WIDTH, WIDTH), (3, 3 * WIDTH, WIDTH // 2), (3, 3 * WIDTH + WIDTH // 2, WIDTH // 2),
          (4, EARLY, STEPS * 6 - EARLY))
LATE = len(PIECES) - 1


def pick(index, values):
    out = jnp.int32(values[0])
    for n, value in enumerate(values[1:], 1):
        out = jnp.where(index == n, jnp.int32(value), out)
    return out


def dot(a, b):
    return jnp.dot(a, b, preferred_element_type=F32)


def dot_t(a, b):
    return lax.dot_general(a, b, (((1,), (1,)), ((), ())), preferred_element_type=F32)


def fold(op, x):
    while x.shape[0] > 8:
        half = x.shape[0] // 2
        x = op(x[:half], x[half:])
    reduce = jnp.max if op is jnp.maximum else jnp.sum
    return reduce(x, axis=0, keepdims=True)


def layer_norm(h, scale, shift):
    mean = jnp.mean(h, axis=-1, keepdims=True)
    cen = h - mean
    var = jnp.mean(cen * cen, axis=-1, keepdims=True)
    return (cen * lax.rsqrt(var + 1e-6) * scale + shift).astype(BF16)


def gelu(x):
    return (0.5 * x) * (1.0 + jnp.tanh(x * (GELU_A + GELU_B * (x * x))))


def kernel(x_ref, hw_ref, sw_ref, win_ref, wout_ref, wqkv_ref, wo_ref, wup_ref, wdown_ref, wskip_ref, mods_ref,
           keep_ref, noise_ref, out_ref, wq, wo, wu, wd, ws, md, chain, outb, wv, h_ref, u_ref, qk_ref, vt_ref, st_ref, top_ref, att_ref,
           act_ref, lat_ref, latt_ref, fin_ref, wsend, wfwd, wrecv, csend, crecv, lsem, fsend, frecv):
    me = lax.axis_index('stage')
    core = lax.rem(me, 2)
    chip = lax.div(me, 2)
    pos = pick(chip, (1, 0, 2, 3))
    next_dev = pick(chip, (2, 0, 3, 3)) * 2 + core
    prev_dev = pick(chip, (1, 1, 0, 2)) * 2 + core
    partner = me + 1 - 2 * core
    first_kind = pick(me, (1, 0, 0, 1, 0, 1, 0, 1))

    held = (wq, wo, wu, wd, md)
    given = (wqkv_ref, wo_ref, wup_ref, wdown_ref, mods_ref)

    def remote(src, dst, send, recv, dev):
        return pltpu.make_async_remote_copy(src_ref=src, dst_ref=dst, send_sem=send, recv_sem=recv,
                                            device_id={'stage': dev}, device_id_type=MESH)

    def source(n):
        arr, row, size = PIECES[n]
        return given[arr].at[pl.ds(row, size)]

    def target(n, kind):
        arr, row, size = PIECES[n]
        return held[arr].at[kind, pl.ds(row, size)]

    for src, dst, kind in MOVES:
        @pl.when(me == src)
        def _():
            for n in range(len(PIECES)):
                remote(source(n), target(n, kind), wsend.at[n], wrecv.at[kind, n], jnp.int32(dst)).start()
    for src, kind in STAYS:
        @pl.when(me == src)
        def _():
            for n in range(len(PIECES)):
                pltpu.make_async_copy(source(n), target(n, kind), wrecv.at[kind, n]).start()

    locals_ = [
        pltpu.make_async_copy(wskip_ref.at[3 - pos], ws, lsem.at[0]),
        pltpu.make_async_copy(hw_ref.at[jnp.maximum(pos - 1, 0), core], chain.at[0, 0], lsem.at[1]),
        pltpu.make_async_copy(hw_ref.at[6 - pos, core], chain.at[1, 0], lsem.at[2]),
        pltpu.make_async_copy(sw_ref.at[pos, core], outb.at[0, SLOTS - 1], lsem.at[3]),
    ]
    for copy in locals_:
        copy.start()
    lat_ref[0] = x_ref[core].T

    def piece_copy(n, kind):
        return remote(target(n, kind), target(n, kind), wfwd.at[n], wrecv.at[kind, n], partner)

    def pass_on(n):
        for kind in range(2):
            @pl.when(first_kind == kind)
            def _():
                piece_copy(n, kind).wait_recv()
                piece_copy(n, kind).start()

    def wait_other(n):
        for kind in range(2):
            @pl.when(first_kind != kind)
            def _():
                piece_copy(n, kind).wait_recv()

    for n in range(3):
        pass_on(n)
    for n in range(3):
        wait_other(n)
    for copy in locals_:
        copy.wait()
    for kind in range(2):
        for n in range(0, WIDTH, NCH):
            wv[kind, n:n + NCH] = wq[kind, :, 2 * WIDTH + n:2 * WIDTH + n + NCH].T
    for n in range(3, LATE):
        pass_on(n)
    for n in range(3, LATE):
        wait_other(n)

    def chain_copy(kind, k, dev):
        s, r = lax.rem(k, SLOTS), lax.rem(k + 1, SLOTS)
        return remote(outb.at[kind, s], chain.at[kind, r], csend.at[kind, s], crecv.at[kind, r], dev)

    low = lax.broadcasted_iota(jnp.int32, (ROWS, 128), 1) < 64

    def split(pair):
        zero = jnp.zeros_like(pair)
        return jnp.where(low, pair, zero), jnp.where(low, zero, pair)

    def item(j, _):
        k = lax.div(j, 2)
        kind = lax.rem(j + core, 2)
        slot = lax.rem(k, SLOTS)
        dest = jnp.where(kind == 0, next_dev, prev_dev)
        has_dest = jnp.where(kind == 0, pos < 3, pos > 0)
        has_src = jnp.where(kind == 0, pos > 0, pos < 3)
        sends = jnp.logical_and(has_dest, k < STEPS - 2 + kind)

        @pl.when(j == 2)
        def _():
            pass_on(LATE)

        @pl.when(j == 4)
        def _():
            wait_other(LATE)

        @pl.when(jnp.logical_and(has_dest, k >= SLOTS))
        def _():
            chain_copy(kind, k, dest).wait_send()

        @pl.when(jnp.logical_and(has_src, k > 0))
        def _():
            chain_copy(kind, k + SLOTS - 1, dest).wait_recv()

        def mod(index):
            return md[kind, k * 6 + index]

        def normalise(first, second):
            for r in range(0, ROWS, LN_ROWS):
                u_ref[r:r + LN_ROWS] = layer_norm(h_ref[r:r + LN_ROWS], 1.0 + mod(first), mod(second))

        @pl.when(jnp.logical_and(kind == 0, pos == 0))
        def _():
            x = lat_ref[lax.rem(k, 2)].astype(BF16)
            h_ref[...] = dot(x, win_ref[...])
            normalise(1, 0)

        @pl.when(jnp.logical_and(kind == 0, pos > 0))
        def _():
            h_ref[...] = chain[0, slot].astype(F32)
            normalise(1, 0)

        @pl.when(kind == 1)
        def _():
            zslot = lax.rem(k + SLOTS - 1, SLOTS)
            for n in range(0, WIDTH, NCH):
                h_ref[:, n:n + NCH] = (dot(chain[1, slot], ws[:WIDTH, n:n + NCH])
                                       + dot(outb[0, zslot], ws[WIDTH:, n:n + NCH]))
            normalise(1, 0)

        def weights(head, q):
            e = jnp.exp2((st_ref[head, :, q:q + 128] - top_ref[head:head + 1, q:q + 128]) * EXP_SCALE)
            return e.astype(BF16), 1.0 / fold(jnp.add, e)

        for n in range(0, 2 * WIDTH, NCH):
            qk_ref[:, n:n + NCH] = dot(u_ref[...], wq[kind, :, n:n + NCH]).astype(BF16)
        for n in range(0, WIDTH, NCH):
            vt_ref[n:n + NCH] = dot_t(wv[kind, n:n + NCH], u_ref[...]).astype(BF16)
        for pair in range(HEADS // 2):
            c = pair * 128
            for half, keys in enumerate(split(qk_ref[:, WIDTH + c:WIDTH + c + 128])):
                head = 2 * pair + half
                s = dot_t(keys, qk_ref[:, c:c + 128])
                st_ref[head] = s
                top_ref[head:head + 1] = fold(jnp.maximum, s)

        @pl.when(j >= 0)
        def _():
            for pair in range(HEADS // 2):
                outs = []
                for head in (2 * pair, 2 * pair + 1):
                    parts = [weights(head, q) for q in (0, 128)]
                    probs = jnp.concatenate([part[0] for part in parts], axis=1)
                    outs.append(dot(vt_ref[head * 64:head * 64 + 64], probs)
                                * jnp.concatenate([part[1] for part in parts], axis=1))
                att_ref[pair] = jnp.concatenate(outs, axis=0).T.astype(BF16)
            att = jnp.concatenate([att_ref[pair] for pair in range(HEADS // 2)], axis=1)
            for n in range(0, WIDTH, NCH):
                h_ref[:, n:n + NCH] += mod(2)[:, n:n + NCH] * dot(att, wo[kind, :, n:n + NCH])

        @pl.when(j >= -2)
        def _():
            normalise(4, 3)
            for n in range(0, HIDDEN, NCH):
                act_ref[:, n:n + NCH] = gelu(dot(u_ref[...], wu[kind, :, n:n + NCH])).astype(BF16)
            for n in range(0, WIDTH, NCH):
                gate = mod(5)[:, n:n + NCH]
                new = h_ref[:, n:n + NCH] + gate * dot(act_ref[:, :HIDDEN // 2], wd[kind, :HIDDEN // 2, n:n + NCH])
                new += gate * dot(act_ref[:, HIDDEN // 2:], wd[kind, HIDDEN // 2:, n:n + NCH])
                outb[kind, slot, :, n:n + NCH] = new.astype(BF16)

        @pl.when(sends)
        def _():
            chain_copy(kind, k, dest).start()

        @pl.when(jnp.logical_and(kind == 0, pos == 3))
        def _():
            chain[1, lax.rem(k + 1, SLOTS)] = outb[0, slot]

        @pl.when(jnp.logical_and(kind == 1, pos == 0))
        def _():
            eps = dot_t(outb[1, slot], wout_ref[...])
            lat_ref[lax.rem(k + 1, 2)] = keep_ref[k] * lat_ref[lax.rem(k, 2)] + noise_ref[k] * eps
        return 0

    def guarded(j, carry):
        skipped = jnp.logical_and(lax.div(j, 2) == STEPS - 1, lax.rem(j + core, 2) == 0)

        @pl.when(jnp.logical_not(skipped))
        def _():
            item(j, 0)
        return carry

    lax.fori_loop(0, 2 * STEPS, guarded, 0)

    for kind, first, last in ((0, STEPS - 5, STEPS - 3), (1, STEPS - 4, STEPS - 2)):
        for k in range(first, last + 1):
            @pl.when(pos < 3 if kind == 0 else pos > 0)
            def _():
                chain_copy(kind, jnp.int32(k), me).wait_send()

    for src, dst, kind in MOVES:
        @pl.when(me == src)
        def _():
            for n in range(len(PIECES)):
                remote(source(n), target(n, kind), wsend.at[n], wrecv.at[kind, n], jnp.int32(dst)).wait_send()
    for n in range(len(PIECES)):
        piece_copy(n, first_kind).wait_send()

    def final_copy(sample, dev):
        return remote(latt_ref, fin_ref.at[sample], fsend.at[dev], frecv.at[sample], jnp.int32(dev))

    for sample in range(2):
        @pl.when(me == 2 + sample)
        def _():
            latt_ref[...] = lat_ref[STEPS % 2].T
            for dev in range(8):
                if dev != 2 + sample:
                    final_copy(sample, dev).start()
            for dev in range(8):
                if dev != 2 + sample:
                    final_copy(sample, dev).wait_send()
            out_ref[sample] = latt_ref[...]

        @pl.when(me != 2 + sample)
        def _():
            final_copy(sample, 0).wait_recv()
            out_ref[sample] = fin_ref[sample]


def solution(mesh):
    assert mesh.shape['stage'] == 8

    def local_run(x_init, h_warm, skip_warm, w_in, w_out, w_qkv, w_o, w_up, w_down, w_skip, ada_mods, keep, noise):
        vmem, hbm, smem = (pl.BlockSpec(memory_space=s) for s in (pltpu.VMEM, pl.ANY, pltpu.SMEM))
        npieces = len(PIECES)
        dma = pltpu.SemaphoreType.DMA
        out = pl.pallas_call(
            kernel,
            out_shape=jax.ShapeDtypeStruct((2, CHANNELS, ROWS), F32),
            in_specs=[vmem, hbm, hbm, vmem, vmem, hbm, hbm, hbm, hbm, hbm, hbm, smem, smem],
            out_specs=vmem,
            scratch_shapes=[
                pltpu.VMEM((2, WIDTH, QKV), BF16), pltpu.VMEM((2, WIDTH, WIDTH), BF16),
                pltpu.VMEM((2, WIDTH, HIDDEN), BF16), pltpu.VMEM((2, HIDDEN, WIDTH), BF16),
                pltpu.VMEM((2 * WIDTH, WIDTH), BF16), pltpu.VMEM((2, STEPS * 6, 1, WIDTH), F32),
                pltpu.VMEM((2, SLOTS, ROWS, WIDTH), BF16), pltpu.VMEM((2, SLOTS, ROWS, WIDTH), BF16),
                pltpu.VMEM((2, WIDTH, WIDTH), BF16),
                pltpu.VMEM((ROWS, WIDTH), F32), pltpu.VMEM((ROWS, WIDTH), BF16), pltpu.VMEM((ROWS, 2 * WIDTH), BF16),
                pltpu.VMEM((WIDTH, ROWS), BF16), pltpu.VMEM((HEADS, ROWS, ROWS), F32), pltpu.VMEM((HEADS, ROWS), F32),
                pltpu.VMEM((HEADS // 2, ROWS, 128), BF16), pltpu.VMEM((ROWS, HIDDEN), BF16),
                pltpu.VMEM((2, ROWS, CHANNELS), F32), pltpu.VMEM((CHANNELS, ROWS), F32),
                pltpu.VMEM((2, CHANNELS, ROWS), F32),
                dma((npieces,)), dma((npieces,)), dma((2, npieces)), dma((2, SLOTS)), dma((2, SLOTS)),
                dma((4,)), dma((8,)), dma((2,)),
            ],
            compiler_params=pltpu.CompilerParams(has_side_effects=True, vmem_limit_bytes=63 * 1024 * 1024),
        )(jnp.transpose(x_init, (0, 2, 1)), h_warm, skip_warm, w_in, w_out.T, w_qkv[0], w_o[0].reshape(WIDTH, WIDTH), w_up[0], w_down[0], w_skip,
          ada_mods.reshape(STEPS * 6, 1, WIDTH), keep, noise)
        return jnp.transpose(out, (0, 2, 1))

    in_specs = (P('data'), P(None, 'data'), P(None, 'data'), P(), P(), P('stage'), P('stage'), P('stage'), P('stage'),
                P(), P(None, 'stage'), P(), P())
    return jax.shard_map(local_run, mesh=mesh, in_specs=in_specs, out_specs=P('data'), check_vma=False)
```

```python
import math

import jax
import jax.numpy as jnp
from jax import lax
from jax.experimental import pallas as pl
from jax.experimental.pallas import tpu as pltpu
from jax.sharding import PartitionSpec as P

MESH = pl.DeviceIdType.MESH
F32, BF16 = jnp.float32, jnp.bfloat16
STEPS, ROWS, WIDTH, HEADS, CHANNELS = 32, 256, 768, 12, 16
QKV, HIDDEN = 3 * WIDTH, 4 * WIDTH
SLOTS = 4
NCH = 256
LN_ROWS = 32
EXP_SCALE = (1.0 / math.sqrt(WIDTH // HEADS)) * math.log2(math.e)
GELU_A = math.sqrt(2.0 / math.pi)
GELU_B = 0.044715 * math.sqrt(2.0 / math.pi)
MOVES = ((0, 2, 0), (2, 4, 0), (3, 6, 0), (4, 7, 1), (6, 0, 1), (7, 3, 1))
STAYS = ((1, 0), (5, 1))
EARLY = 2 * 6
PIECES = ((4, 0, EARLY), (0, 0, WIDTH), (1, 0, WIDTH), (2, 0, WIDTH), (3, 0, WIDTH), (3, WIDTH, WIDTH),
          (3, 2 * WIDTH, WIDTH), (3, 3 * WIDTH, WIDTH // 2), (3, 3 * WIDTH + WIDTH // 2, WIDTH // 2),
          (4, EARLY, STEPS * 6 - EARLY))
LATE = len(PIECES) - 1


def pick(index, values):
    out = jnp.int32(values[0])
    for n, value in enumerate(values[1:], 1):
        out = jnp.where(index == n, jnp.int32(value), out)
    return out


def dot(a, b):
    return jnp.dot(a, b, preferred_element_type=F32)


def dot_t(a, b):
    return lax.dot_general(a, b, (((1,), (1,)), ((), ())), preferred_element_type=F32)


def fold(op, x):
    while x.shape[0] > 8:
        half = x.shape[0] // 2
        x = op(x[:half], x[half:])
    reduce = jnp.max if op is jnp.maximum else jnp.sum
    return reduce(x, axis=0, keepdims=True)


def layer_norm(h, scale, shift):
    mean = jnp.mean(h, axis=-1, keepdims=True)
    cen = h - mean
    var = jnp.mean(cen * cen, axis=-1, keepdims=True)
    return (cen * lax.rsqrt(var + 1e-6) * scale + shift).astype(BF16)


def gelu(x):
    return (0.5 * x) * (1.0 + jnp.tanh(x * (GELU_A + GELU_B * (x * x))))


def kernel(x_ref, hw_ref, sw_ref, win_ref, wout_ref, wqkv_ref, wo_ref, wup_ref, wdown_ref, wskip_ref, mods_ref,
           keep_ref, noise_ref, out_ref, wq, wo, wu, wd, ws, md, chain, outb, wv, h_ref, u_ref, qk_ref, vt_ref, st_ref, top_ref, att_ref,
           act_ref, lat_ref, latt_ref, fin_ref, wsend, wfwd, wrecv, csend, crecv, lsem, fsend, frecv):
    me = lax.axis_index('stage')
    core = lax.rem(me, 2)
    chip = lax.div(me, 2)
    pos = pick(chip, (1, 0, 2, 3))
    next_dev = pick(chip, (2, 0, 3, 3)) * 2 + core
    prev_dev = pick(chip, (1, 1, 0, 2)) * 2 + core
    partner = me + 1 - 2 * core
    first_kind = pick(me, (1, 0, 0, 1, 0, 1, 0, 1))

    held = (wq, wo, wu, wd, md)
    given = (wqkv_ref, wo_ref, wup_ref, wdown_ref, mods_ref)

    def remote(src, dst, send, recv, dev):
        return pltpu.make_async_remote_copy(src_ref=src, dst_ref=dst, send_sem=send, recv_sem=recv,
                                            device_id={'stage': dev}, device_id_type=MESH)

    def source(n):
        arr, row, size = PIECES[n]
        return given[arr].at[pl.ds(row, size)]

    def target(n, kind):
        arr, row, size = PIECES[n]
        return held[arr].at[kind, pl.ds(row, size)]

    for src, dst, kind in MOVES:
        @pl.when(me == src)
        def _():
            for n in range(len(PIECES)):
                remote(source(n), target(n, kind), wsend.at[n], wrecv.at[kind, n], jnp.int32(dst)).start()
    for src, kind in STAYS:
        @pl.when(me == src)
        def _():
            for n in range(len(PIECES)):
                pltpu.make_async_copy(source(n), target(n, kind), wrecv.at[kind, n]).start()

    locals_ = [
        pltpu.make_async_copy(wskip_ref.at[3 - pos], ws, lsem.at[0]),
        pltpu.make_async_copy(hw_ref.at[jnp.maximum(pos - 1, 0), core], chain.at[0, 0], lsem.at[1]),
        pltpu.make_async_copy(hw_ref.at[6 - pos, core], chain.at[1, 0], lsem.at[2]),
        pltpu.make_async_copy(sw_ref.at[pos, core], outb.at[0, SLOTS - 1], lsem.at[3]),
    ]
    for copy in locals_:
        copy.start()
    lat_ref[0] = x_ref[core].T

    def piece_copy(n, kind):
        return remote(target(n, kind), target(n, kind), wfwd.at[n], wrecv.at[kind, n], partner)

    def pass_on(n):
        for kind in range(2):
            @pl.when(first_kind == kind)
            def _():
                piece_copy(n, kind).wait_recv()
                piece_copy(n, kind).start()

    def wait_other(n):
        for kind in range(2):
            @pl.when(first_kind != kind)
            def _():
                piece_copy(n, kind).wait_recv()

    for n in range(3):
        pass_on(n)
    for n in range(3):
        wait_other(n)
    for copy in locals_:
        copy.wait()
    for kind in range(2):
        for n in range(0, WIDTH, NCH):
            wv[kind, n:n + NCH] = wq[kind, :, 2 * WIDTH + n:2 * WIDTH + n + NCH].T
    for n in range(3, LATE):
        pass_on(n)
    for n in range(3, LATE):
        wait_other(n)

    def chain_copy(kind, k, dev):
        s, r = lax.rem(k, SLOTS), lax.rem(k + 1, SLOTS)
        return remote(outb.at[kind, s], chain.at[kind, r], csend.at[kind, s], crecv.at[kind, r], dev)

    low = lax.broadcasted_iota(jnp.int32, (ROWS, 128), 1) < 64

    def split(pair):
        zero = jnp.zeros_like(pair)
        return jnp.where(low, pair, zero), jnp.where(low, zero, pair)

    def item(j, _):
        k = lax.div(j, 2)
        kind = lax.rem(j + core, 2)
        slot = lax.rem(k, SLOTS)
        dest = jnp.where(kind == 0, next_dev, prev_dev)
        has_dest = jnp.where(kind == 0, pos < 3, pos > 0)
        has_src = jnp.where(kind == 0, pos > 0, pos < 3)
        sends = jnp.logical_and(has_dest, k < STEPS - 2 + kind)

        @pl.when(j == 2)
        def _():
            pass_on(LATE)

        @pl.when(j == 4)
        def _():
            wait_other(LATE)

        @pl.when(jnp.logical_and(has_dest, k >= SLOTS))
        def _():
            chain_copy(kind, k, dest).wait_send()

        @pl.when(kind == 1)
        def _():
            zslot = lax.rem(k + SLOTS - 1, SLOTS)
            for n in range(0, WIDTH, NCH):
                h_ref[:, n:n + NCH] = dot(outb[0, zslot], ws[WIDTH:, n:n + NCH])

        @pl.when(jnp.logical_and(has_src, k > 0))
        def _():
            chain_copy(kind, k + SLOTS - 1, dest).wait_recv()

        @pl.when(jnp.logical_and(kind == 0, pos == 0))
        def _():
            x = lat_ref[lax.rem(k, 2)].astype(BF16)
            h_ref[...] = dot(x, win_ref[...])

        @pl.when(jnp.logical_and(kind == 0, pos > 0))
        def _():
            h_ref[...] = chain[0, slot].astype(F32)

        @pl.when(kind == 1)
        def _():
            for n in range(0, WIDTH, NCH):
                h_ref[:, n:n + NCH] += dot(chain[1, slot], ws[:WIDTH, n:n + NCH])

        def mod(index):
            return md[kind, k * 6 + index]

        for r in range(0, ROWS, LN_ROWS):
            u_ref[r:r + LN_ROWS] = layer_norm(h_ref[r:r + LN_ROWS], 1.0 + mod(1), mod(0))
        def weights(head, q):
            e = jnp.exp2((st_ref[head, :, q:q + 128] - top_ref[head:head + 1, q:q + 128]) * EXP_SCALE)
            return e.astype(BF16), 1.0 / fold(jnp.add, e)

        for n in range(0, 2 * WIDTH, NCH):
            qk_ref[:, n:n + NCH] = dot(u_ref[...], wq[kind, :, n:n + NCH]).astype(BF16)
        for n in range(0, WIDTH, NCH):
            vt_ref[n:n + NCH] = dot_t(wv[kind, n:n + NCH], u_ref[...]).astype(BF16)
        for pair in range(HEADS // 2):
            c = pair * 128
            for half, keys in enumerate(split(qk_ref[:, WIDTH + c:WIDTH + c + 128])):
                head = 2 * pair + half
                s = dot_t(keys, qk_ref[:, c:c + 128])
                st_ref[head] = s
                top_ref[head:head + 1] = fold(jnp.maximum, s)

        @pl.when(j >= 0)
        def _():
            for pair in range(HEADS // 2):
                outs = []
                for head in (2 * pair, 2 * pair + 1):
                    parts = [weights(head, q) for q in (0, 128)]
                    probs = jnp.concatenate([part[0] for part in parts], axis=1)
                    outs.append(dot(vt_ref[head * 64:head * 64 + 64], probs)
                                * jnp.concatenate([part[1] for part in parts], axis=1))
                att_ref[pair] = jnp.concatenate(outs, axis=0).T.astype(BF16)
            att = jnp.concatenate([att_ref[pair] for pair in range(HEADS // 2)], axis=1)
            for n in range(0, WIDTH, NCH):
                h_ref[:, n:n + NCH] += mod(2)[:, n:n + NCH] * dot(att, wo[kind, :, n:n + NCH])
            for r in range(0, ROWS, LN_ROWS):
                u_ref[r:r + LN_ROWS] = layer_norm(h_ref[r:r + LN_ROWS], 1.0 + mod(4), mod(3))
            for n in range(0, HIDDEN, NCH):
                act_ref[:, n:n + NCH] = gelu(dot(u_ref[...], wu[kind, :, n:n + NCH])).astype(BF16)
            for n in range(0, WIDTH, NCH):
                gate = mod(5)[:, n:n + NCH]
                new = h_ref[:, n:n + NCH] + gate * dot(act_ref[:, :HIDDEN // 2], wd[kind, :HIDDEN // 2, n:n + NCH])
                new += gate * dot(act_ref[:, HIDDEN // 2:], wd[kind, HIDDEN // 2:, n:n + NCH])
                outb[kind, slot, :, n:n + NCH] = new.astype(BF16)

        @pl.when(sends)
        def _():
            chain_copy(kind, k, dest).start()

        @pl.when(jnp.logical_and(kind == 0, pos == 3))
        def _():
            chain[1, lax.rem(k + 1, SLOTS)] = outb[0, slot]

        @pl.when(jnp.logical_and(kind == 1, pos == 0))
        def _():
            eps = dot_t(outb[1, slot], wout_ref[...])
            lat_ref[lax.rem(k + 1, 2)] = keep_ref[k] * lat_ref[lax.rem(k, 2)] + noise_ref[k] * eps
        return 0

    def guarded(j, carry):
        skipped = jnp.logical_and(lax.div(j, 2) == STEPS - 1, lax.rem(j + core, 2) == 0)

        @pl.when(jnp.logical_not(skipped))
        def _():
            item(j, 0)
        return carry

    lax.fori_loop(0, 2 * STEPS, guarded, 0)

    for kind, first, last in ((0, STEPS - 5, STEPS - 3), (1, STEPS - 4, STEPS - 2)):
        for k in range(first, last + 1):
            @pl.when(pos < 3 if kind == 0 else pos > 0)
            def _():
                chain_copy(kind, jnp.int32(k), me).wait_send()

    for src, dst, kind in MOVES:
        @pl.when(me == src)
        def _():
            for n in range(len(PIECES)):
                remote(source(n), target(n, kind), wsend.at[n], wrecv.at[kind, n], jnp.int32(dst)).wait_send()
    for n in range(len(PIECES)):
        piece_copy(n, first_kind).wait_send()

    def final_copy(sample, dev):
        return remote(latt_ref, fin_ref.at[sample], fsend.at[dev], frecv.at[sample], jnp.int32(dev))

    for sample in range(2):
        @pl.when(me == 2 + sample)
        def _():
            latt_ref[...] = lat_ref[STEPS % 2].T
            for dev in range(8):
                if dev != 2 + sample:
                    final_copy(sample, dev).start()
            for dev in range(8):
                if dev != 2 + sample:
                    final_copy(sample, dev).wait_send()
            out_ref[sample] = latt_ref[...]

        @pl.when(me != 2 + sample)
        def _():
            final_copy(sample, 0).wait_recv()
            out_ref[sample] = fin_ref[sample]


def solution(mesh):
    assert mesh.shape['stage'] == 8

    def local_run(x_init, h_warm, skip_warm, w_in, w_out, w_qkv, w_o, w_up, w_down, w_skip, ada_mods, keep, noise):
        vmem, hbm, smem = (pl.BlockSpec(memory_space=s) for s in (pltpu.VMEM, pl.ANY, pltpu.SMEM))
        npieces = len(PIECES)
        dma = pltpu.SemaphoreType.DMA
        out = pl.pallas_call(
            kernel,
            out_shape=jax.ShapeDtypeStruct((2, CHANNELS, ROWS), F32),
            in_specs=[vmem, hbm, hbm, vmem, vmem, hbm, hbm, hbm, hbm, hbm, hbm, smem, smem],
            out_specs=vmem,
            scratch_shapes=[
                pltpu.VMEM((2, WIDTH, QKV), BF16), pltpu.VMEM((2, WIDTH, WIDTH), BF16),
                pltpu.VMEM((2, WIDTH, HIDDEN), BF16), pltpu.VMEM((2, HIDDEN, WIDTH), BF16),
                pltpu.VMEM((2 * WIDTH, WIDTH), BF16), pltpu.VMEM((2, STEPS * 6, 1, WIDTH), F32),
                pltpu.VMEM((2, SLOTS, ROWS, WIDTH), BF16), pltpu.VMEM((2, SLOTS, ROWS, WIDTH), BF16),
                pltpu.VMEM((2, WIDTH, WIDTH), BF16),
                pltpu.VMEM((ROWS, WIDTH), F32), pltpu.VMEM((ROWS, WIDTH), BF16), pltpu.VMEM((ROWS, 2 * WIDTH), BF16),
                pltpu.VMEM((WIDTH, ROWS), BF16), pltpu.VMEM((HEADS, ROWS, ROWS), F32), pltpu.VMEM((HEADS, ROWS), F32),
                pltpu.VMEM((HEADS // 2, ROWS, 128), BF16), pltpu.VMEM((ROWS, HIDDEN), BF16),
                pltpu.VMEM((2, ROWS, CHANNELS), F32), pltpu.VMEM((CHANNELS, ROWS), F32),
                pltpu.VMEM((2, CHANNELS, ROWS), F32),
                dma((npieces,)), dma((npieces,)), dma((2, npieces)), dma((2, SLOTS)), dma((2, SLOTS)),
                dma((4,)), dma((8,)), dma((2,)),
            ],
            compiler_params=pltpu.CompilerParams(has_side_effects=True, vmem_limit_bytes=63 * 1024 * 1024),
        )(jnp.transpose(x_init, (0, 2, 1)), h_warm, skip_warm, w_in, w_out.T, w_qkv[0], w_o[0].reshape(WIDTH, WIDTH), w_up[0], w_down[0], w_skip,
          ada_mods.reshape(STEPS * 6, 1, WIDTH), keep, noise)
        return jnp.transpose(out, (0, 2, 1))

    in_specs = (P('data'), P(None, 'data'), P(None, 'data'), P(), P(), P('stage'), P('stage'), P('stage'), P('stage'),
                P(), P(None, 'stage'), P(), P())
    return jax.shard_map(local_run, mesh=mesh, in_specs=in_specs, out_specs=P('data'), check_vma=False)
```

```python
import math

import jax
import jax.numpy as jnp
from jax import lax
from jax.experimental import pallas as pl
from jax.experimental.pallas import tpu as pltpu
from jax.sharding import PartitionSpec as P

MESH = pl.DeviceIdType.MESH
F32, BF16 = jnp.float32, jnp.bfloat16
STEPS, ROWS, WIDTH, HEADS, CHANNELS = 32, 256, 768, 12, 16
QKV, HIDDEN = 3 * WIDTH, 4 * WIDTH
SLOTS = 4
NCH = 256
LN_ROWS = 32
EXP_SCALE = (1.0 / math.sqrt(WIDTH // HEADS)) * math.log2(math.e)
GELU_A = math.sqrt(2.0 / math.pi)
GELU_B = 0.044715 * math.sqrt(2.0 / math.pi)
MOVES = ((0, 2, 0), (2, 4, 0), (3, 6, 0), (4, 7, 1), (6, 0, 1), (7, 3, 1))
STAYS = ((1, 0), (5, 1))
EARLY = 2 * 6
PIECES = ((4, 0, EARLY), (0, 0, WIDTH), (1, 0, WIDTH), (2, 0, WIDTH), (3, 0, WIDTH), (3, WIDTH, WIDTH),
          (3, 2 * WIDTH, WIDTH), (3, 3 * WIDTH, WIDTH // 2),
          (3, 3 * WIDTH + WIDTH // 2, WIDTH // 4), (3, 3 * WIDTH + 3 * WIDTH // 4, WIDTH // 4),
          (4, EARLY, STEPS * 6 - EARLY))
LATE = len(PIECES) - 1


def pick(index, values):
    out = jnp.int32(values[0])
    for n, value in enumerate(values[1:], 1):
        out = jnp.where(index == n, jnp.int32(value), out)
    return out


def dot(a, b):
    return jnp.dot(a, b, preferred_element_type=F32)


def dot_t(a, b):
    return lax.dot_general(a, b, (((1,), (1,)), ((), ())), preferred_element_type=F32)


def fold(op, x):
    while x.shape[0] > 8:
        half = x.shape[0] // 2
        x = op(x[:half], x[half:])
    reduce = jnp.max if op is jnp.maximum else jnp.sum
    return reduce(x, axis=0, keepdims=True)


def layer_norm(h, scale, shift):
    mean = jnp.mean(h, axis=-1, keepdims=True)
    cen = h - mean
    var = jnp.mean(cen * cen, axis=-1, keepdims=True)
    return (cen * lax.rsqrt(var + 1e-6) * scale + shift).astype(BF16)


def gelu(x):
    return (0.5 * x) * (1.0 + jnp.tanh(x * (GELU_A + GELU_B * (x * x))))


def kernel(x_ref, hw_ref, sw_ref, win_ref, wout_ref, wqkv_ref, wo_ref, wup_ref, wdown_ref, wskip_ref, mods_ref,
           keep_ref, noise_ref, out_ref, wq, wo, wu, wd, ws, md, chain, outb, wv, h_ref, u_ref, qk_ref, vt_ref, st_ref, top_ref, att_ref,
           act_ref, lat_ref, latt_ref, fin_ref, wsend, wfwd, wrecv, csend, crecv, lsem, fsend, frecv):
    me = lax.axis_index('stage')
    core = lax.rem(me, 2)
    chip = lax.div(me, 2)
    pos = pick(chip, (1, 0, 2, 3))
    next_dev = pick(chip, (2, 0, 3, 3)) * 2 + core
    prev_dev = pick(chip, (1, 1, 0, 2)) * 2 + core
    partner = me + 1 - 2 * core
    first_kind = pick(me, (1, 0, 0, 1, 0, 1, 0, 1))

    held = (wq, wo, wu, wd, md)
    given = (wqkv_ref, wo_ref, wup_ref, wdown_ref, mods_ref)

    def remote(src, dst, send, recv, dev):
        return pltpu.make_async_remote_copy(src_ref=src, dst_ref=dst, send_sem=send, recv_sem=recv,
                                            device_id={'stage': dev}, device_id_type=MESH)

    def source(n):
        arr, row, size = PIECES[n]
        return given[arr].at[pl.ds(row, size)]

    def target(n, kind):
        arr, row, size = PIECES[n]
        return held[arr].at[kind, pl.ds(row, size)]

    for src, dst, kind in MOVES:
        @pl.when(me == src)
        def _():
            for n in range(len(PIECES)):
                remote(source(n), target(n, kind), wsend.at[n], wrecv.at[kind, n], jnp.int32(dst)).start()
    for src, kind in STAYS:
        @pl.when(me == src)
        def _():
            for n in range(len(PIECES)):
                pltpu.make_async_copy(source(n), target(n, kind), wrecv.at[kind, n]).start()

    locals_ = [
        pltpu.make_async_copy(wskip_ref.at[3 - pos], ws, lsem.at[0]),
        pltpu.make_async_copy(hw_ref.at[jnp.maximum(pos - 1, 0), core], chain.at[0, 0], lsem.at[1]),
        pltpu.make_async_copy(hw_ref.at[6 - pos, core], chain.at[1, 0], lsem.at[2]),
        pltpu.make_async_copy(sw_ref.at[pos, core], outb.at[0, SLOTS - 1], lsem.at[3]),
    ]
    for copy in locals_:
        copy.start()
    lat_ref[0] = x_ref[core].T

    def piece_copy(n, kind):
        return remote(target(n, kind), target(n, kind), wfwd.at[n], wrecv.at[kind, n], partner)

    def pass_on(n):
        for kind in range(2):
            @pl.when(first_kind == kind)
            def _():
                piece_copy(n, kind).wait_recv()
                piece_copy(n, kind).start()

    def wait_other(n):
        for kind in range(2):
            @pl.when(first_kind != kind)
            def _():
                piece_copy(n, kind).wait_recv()

    for n in range(3):
        pass_on(n)
    for n in range(3):
        wait_other(n)
    for copy in locals_:
        copy.wait()
    for kind in range(2):
        for n in range(0, WIDTH, NCH):
            wv[kind, n:n + NCH] = wq[kind, :, 2 * WIDTH + n:2 * WIDTH + n + NCH].T
    for n in range(3, LATE):
        pass_on(n)
    for n in range(3, LATE):
        wait_other(n)

    def chain_copy(kind, k, dev):
        s, r = lax.rem(k, SLOTS), lax.rem(k + 1, SLOTS)
        return remote(outb.at[kind, s], chain.at[kind, r], csend.at[kind, s], crecv.at[kind, r], dev)

    low = lax.broadcasted_iota(jnp.int32, (ROWS, 128), 1) < 64

    def split(pair):
        zero = jnp.zeros_like(pair)
        return jnp.where(low, pair, zero), jnp.where(low, zero, pair)

    def item(j, _):
        k = lax.div(j, 2)
        kind = lax.rem(j + core, 2)
        slot = lax.rem(k, SLOTS)
        dest = jnp.where(kind == 0, next_dev, prev_dev)
        has_dest = jnp.where(kind == 0, pos < 3, pos > 0)
        has_src = jnp.where(kind == 0, pos > 0, pos < 3)
        sends = jnp.logical_and(has_dest, k < STEPS - 2 + kind)

        @pl.when(j == 2)
        def _():
            pass_on(LATE)

        @pl.when(j == 4)
        def _():
            wait_other(LATE)

        @pl.when(jnp.logical_and(has_dest, k >= SLOTS))
        def _():
            chain_copy(kind, k, dest).wait_send()

        @pl.when(kind == 1)
        def _():
            zslot = lax.rem(k + SLOTS - 1, SLOTS)
            for n in range(0, WIDTH, NCH):
                h_ref[:, n:n + NCH] = dot(outb[0, zslot], ws[WIDTH:, n:n + NCH])

        @pl.when(jnp.logical_and(has_src, k > 0))
        def _():
            chain_copy(kind, k + SLOTS - 1, dest).wait_recv()

        @pl.when(jnp.logical_and(kind == 0, pos == 0))
        def _():
            x = lat_ref[lax.rem(k, 2)].astype(BF16)
            h_ref[...] = dot(x, win_ref[...])

        @pl.when(jnp.logical_and(kind == 0, pos > 0))
        def _():
            h_ref[...] = chain[0, slot].astype(F32)

        @pl.when(kind == 1)
        def _():
            for n in range(0, WIDTH, NCH):
                h_ref[:, n:n + NCH] += dot(chain[1, slot], ws[:WIDTH, n:n + NCH])

        def mod(index):
            return md[kind, k * 6 + index]

        for r in range(0, ROWS, LN_ROWS):
            u_ref[r:r + LN_ROWS] = layer_norm(h_ref[r:r + LN_ROWS], 1.0 + mod(1), mod(0))
        def weights(head, q):
            e = jnp.exp2((st_ref[head, :, q:q + 128] - top_ref[head:head + 1, q:q + 128]) * EXP_SCALE)
            return e.astype(BF16), 1.0 / fold(jnp.add, e)

        for n in range(0, 2 * WIDTH, NCH):
            qk_ref[:, n:n + NCH] = dot(u_ref[...], wq[kind, :, n:n + NCH]).astype(BF16)
        for n in range(0, WIDTH, NCH):
            vt_ref[n:n + NCH] = dot_t(wv[kind, n:n + NCH], u_ref[...]).astype(BF16)
        for pair in range(HEADS // 2):
            c = pair * 128
            for half, keys in enumerate(split(qk_ref[:, WIDTH + c:WIDTH + c + 128])):
                head = 2 * pair + half
                s = dot_t(keys, qk_ref[:, c:c + 128])
                st_ref[head] = s
                top_ref[head:head + 1] = fold(jnp.maximum, s)

        @pl.when(j >= 0)
        def _():
            for pair in range(HEADS // 2):
                outs = []
                for head in (2 * pair, 2 * pair + 1):
                    parts = [weights(head, q) for q in (0, 128)]
                    probs = jnp.concatenate([part[0] for part in parts], axis=1)
                    outs.append(dot(vt_ref[head * 64:head * 64 + 64], probs)
                                * jnp.concatenate([part[1] for part in parts], axis=1))
                att_ref[pair] = jnp.concatenate(outs, axis=0).T.astype(BF16)
            att = jnp.concatenate([att_ref[pair] for pair in range(HEADS // 2)], axis=1)
            for n in range(0, WIDTH, NCH):
                h_ref[:, n:n + NCH] += mod(2)[:, n:n + NCH] * dot(att, wo[kind, :, n:n + NCH])
            for r in range(0, ROWS, LN_ROWS):
                u_ref[r:r + LN_ROWS] = layer_norm(h_ref[r:r + LN_ROWS], 1.0 + mod(4), mod(3))
            for n in range(0, HIDDEN, NCH):
                act_ref[:, n:n + NCH] = gelu(dot(u_ref[...], wu[kind, :, n:n + NCH])).astype(BF16)
            for n in range(0, WIDTH, NCH):
                gate = mod(5)[:, n:n + NCH]
                new = h_ref[:, n:n + NCH] + gate * dot(act_ref[:, :HIDDEN // 2], wd[kind, :HIDDEN // 2, n:n + NCH])
                new += gate * dot(act_ref[:, HIDDEN // 2:], wd[kind, HIDDEN // 2:, n:n + NCH])
                outb[kind, slot, :, n:n + NCH] = new.astype(BF16)

        @pl.when(sends)
        def _():
            chain_copy(kind, k, dest).start()

        @pl.when(jnp.logical_and(kind == 0, pos == 3))
        def _():
            chain[1, lax.rem(k + 1, SLOTS)] = outb[0, slot]

        @pl.when(jnp.logical_and(kind == 1, pos == 0))
        def _():
            eps = dot_t(outb[1, slot], wout_ref[...])
            lat_ref[lax.rem(k + 1, 2)] = keep_ref[k] * lat_ref[lax.rem(k, 2)] + noise_ref[k] * eps
        return 0

    def guarded(j, carry):
        skipped = jnp.logical_and(lax.div(j, 2) == STEPS - 1, lax.rem(j + core, 2) == 0)

        @pl.when(jnp.logical_not(skipped))
        def _():
            item(j, 0)
        return carry

    lax.fori_loop(0, 2 * STEPS, guarded, 0)

    for kind, first, last in ((0, STEPS - 5, STEPS - 3), (1, STEPS - 4, STEPS - 2)):
        for k in range(first, last + 1):
            @pl.when(pos < 3 if kind == 0 else pos > 0)
            def _():
                chain_copy(kind, jnp.int32(k), me).wait_send()

    for src, dst, kind in MOVES:
        @pl.when(me == src)
        def _():
            for n in range(len(PIECES)):
                remote(source(n), target(n, kind), wsend.at[n], wrecv.at[kind, n], jnp.int32(dst)).wait_send()
    for n in range(len(PIECES)):
        piece_copy(n, first_kind).wait_send()

    def final_copy(sample, dev):
        return remote(latt_ref, fin_ref.at[sample], fsend.at[dev], frecv.at[sample], jnp.int32(dev))

    for sample in range(2):
        @pl.when(me == 2 + sample)
        def _():
            latt_ref[...] = lat_ref[STEPS % 2].T
            for dev in range(8):
                if dev != 2 + sample:
                    final_copy(sample, dev).start()
            for dev in range(8):
                if dev != 2 + sample:
                    final_copy(sample, dev).wait_send()
            out_ref[sample] = latt_ref[...]

        @pl.when(me != 2 + sample)
        def _():
            final_copy(sample, 0).wait_recv()
            out_ref[sample] = fin_ref[sample]


def solution(mesh):
    assert mesh.shape['stage'] == 8

    def local_run(x_init, h_warm, skip_warm, w_in, w_out, w_qkv, w_o, w_up, w_down, w_skip, ada_mods, keep, noise):
        vmem, hbm, smem = (pl.BlockSpec(memory_space=s) for s in (pltpu.VMEM, pl.ANY, pltpu.SMEM))
        npieces = len(PIECES)
        dma = pltpu.SemaphoreType.DMA
        out = pl.pallas_call(
            kernel,
            out_shape=jax.ShapeDtypeStruct((2, CHANNELS, ROWS), F32),
            in_specs=[vmem, hbm, hbm, vmem, vmem, hbm, hbm, hbm, hbm, hbm, hbm, smem, smem],
            out_specs=vmem,
            scratch_shapes=[
                pltpu.VMEM((2, WIDTH, QKV), BF16), pltpu.VMEM((2, WIDTH, WIDTH), BF16),
                pltpu.VMEM((2, WIDTH, HIDDEN), BF16), pltpu.VMEM((2, HIDDEN, WIDTH), BF16),
                pltpu.VMEM((2 * WIDTH, WIDTH), BF16), pltpu.VMEM((2, STEPS * 6, 1, WIDTH), F32),
                pltpu.VMEM((2, SLOTS, ROWS, WIDTH), BF16), pltpu.VMEM((2, SLOTS, ROWS, WIDTH), BF16),
                pltpu.VMEM((2, WIDTH, WIDTH), BF16),
                pltpu.VMEM((ROWS, WIDTH), F32), pltpu.VMEM((ROWS, WIDTH), BF16), pltpu.VMEM((ROWS, 2 * WIDTH), BF16),
                pltpu.VMEM((WIDTH, ROWS), BF16), pltpu.VMEM((HEADS, ROWS, ROWS), F32), pltpu.VMEM((HEADS, ROWS), F32),
                pltpu.VMEM((HEADS // 2, ROWS, 128), BF16), pltpu.VMEM((ROWS, HIDDEN), BF16),
                pltpu.VMEM((2, ROWS, CHANNELS), F32), pltpu.VMEM((CHANNELS, ROWS), F32),
                pltpu.VMEM((2, CHANNELS, ROWS), F32),
                dma((npieces,)), dma((npieces,)), dma((2, npieces)), dma((2, SLOTS)), dma((2, SLOTS)),
                dma((4,)), dma((8,)), dma((2,)),
            ],
            compiler_params=pltpu.CompilerParams(has_side_effects=True, vmem_limit_bytes=63 * 1024 * 1024),
        )(jnp.transpose(x_init, (0, 2, 1)), h_warm, skip_warm, w_in, w_out.T, w_qkv[0], w_o[0].reshape(WIDTH, WIDTH), w_up[0], w_down[0], w_skip,
          ada_mods.reshape(STEPS * 6, 1, WIDTH), keep, noise)
        return jnp.transpose(out, (0, 2, 1))

    in_specs = (P('data'), P(None, 'data'), P(None, 'data'), P(), P(), P('stage'), P('stage'), P('stage'), P('stage'),
                P(), P(None, 'stage'), P(), P())
    return jax.shard_map(local_run, mesh=mesh, in_specs=in_specs, out_specs=P('data'), check_vma=False)
```
